32 devices in a mesh: gx: 8 (over z, core), gy: 4 (over y, x).
Axes of the slice: x: 2, y: 2, z: 4, core: 2. Of those that a mesh axis runs over, the one named last changes fastest.
Arguments:
- earlier_heat_field: float32 [6, 1024, 512], P(None, 'gx', 'gy'), may hold values from -6 to 6
- substance_per_voxel: int32 [6, 1024, 512], P(None, 'gx', 'gy'), may hold values from 0 to 7
- patch_wattage_category: int32 [64, 32], P('gx', 'gy'), may hold values from 0 to 63
- planar_coupling: float32 [8], replicated, may hold values from 0.3 to 3
- vertical_coupling_per_substance: float32 [8], replicated, may hold values from 0.05 to 0.5
- heat_mass_ratio: float32 [8], replicated, may hold values from 2e-05 to 0.0002
- wattage_per_category: float32 [64], replicated, may hold values from 2e-06 to 2e-05
Outputs:
- temperature: float32 [6, 1024, 512], P(None, 'gx', 'gy')
The draws below stay inside these ranges and needn't reach their ends.
All inputs are finite; a program needn't handle non-finite values.
Results may differ from the reference program's by a relative error of at most 0.0003.
Values sent between devices are 32-bit elements; how exact they have to be, the bound alone decides.
A program may use at most 192 MiB of HBM per device.

```python
import math
import jax
import jax.numpy as jnp
from jax import lax

DIE_COUNT = 6
MATERIALS = 8
POWER_LEVELS = 64
TILE = 16
LEVELS = 6
SWEEPS = 2
COARSE_ITERS = 12
CX = 128
GRID_LENGTH = 1024
GRID_WIDTH = 512


def draw_substance_per_voxel(key, part):
    block_key = jax.random.fold_in(key, 11)
    noise_key = jax.random.fold_in(key, 23)
    pick_key = jax.random.fold_in(key, 37)
    blocks = jax.random.randint(block_key, (DIE_COUNT, GRID_LENGTH // CX, GRID_WIDTH // CX), 0, MATERIALS)
    spread = jnp.repeat(jnp.repeat(blocks, CX, axis=1), CX, axis=2)
    shape = (DIE_COUNT, GRID_LENGTH, GRID_WIDTH)
    noise = jax.random.randint(noise_key, shape, 0, MATERIALS)
    pick = jax.random.randint(pick_key, shape, 0, 4)
    return jnp.where(pick == 0, noise, spread).astype(jnp.int32)


def plant(values, stream_key, smallest, high):
    dims = values.shape
    place = [jax.random.randint(jax.random.fold_in(stream_key, axis), (), 0, dims[axis]) for axis in range(len(dims))]
    values = values.at[tuple(place)].set(smallest)
    longest = dims.index(max(dims))
    place[longest] = (place[longest] + 1) % dims[longest]
    return values.at[tuple(place)].set(high)


def shard_levels(rng, dims, shards, least, top_value):
    loudness, own = 1.0, jax.random.fold_in(rng, 6)
    for axis_at, blocks in shards:
        draws = jnp.exp(jax.random.uniform(jax.random.fold_in(own, axis_at), (blocks,), jnp.float32, least / len(shards), top_value / len(shards)))
        loudness = loudness * jnp.repeat(draws, dims[axis_at] // blocks).reshape([-1 if axis == axis_at else 1 for axis in range(len(dims))])
    return loudness


def scatter_about(own_key, dims, width, limit, shards=(), held_as=jnp.bfloat16):
    loudness = shard_levels(own_key, dims, shards, -0.22, 0.18) if shards else 1.0
    values = jax.random.normal(own_key, dims, jnp.float32) * width * loudness
    return jnp.minimum(jnp.maximum(values, -limit), limit).astype(held_as)


def setup_inputs(seed: int = 0) -> dict:
    seeds = jax.random.split(jax.random.key(seed), 8)
    return {
        "earlier_heat_field": scatter_about(seeds[0], (DIE_COUNT, GRID_LENGTH, GRID_WIDTH), 1.0, 6.0, ((1, 8), (2, 4)), jnp.float32),
        "substance_per_voxel": draw_substance_per_voxel(jax.random.fold_in(seeds[7], 71), 0),
        "patch_wattage_category": plant(jax.random.randint(seeds[2], (GRID_LENGTH // TILE, GRID_WIDTH // TILE), 0, POWER_LEVELS), jax.random.fold_in(seeds[2], 1), 0, POWER_LEVELS - 1).astype(jnp.int32),
        "planar_coupling": jnp.clip(jnp.exp(jax.random.uniform(seeds[3], (MATERIALS,), jnp.float32, math.log(0.3), math.log(3.0))), 0.3, 3.0),
        "vertical_coupling_per_substance": jnp.clip(jnp.exp(jax.random.uniform(seeds[4], (MATERIALS,), jnp.float32, math.log(0.05), math.log(0.5))), 0.05, 0.5),
        "heat_mass_ratio": jnp.clip(jnp.exp(jax.random.uniform(seeds[5], (MATERIALS,), jnp.float32, math.log(1.9999999494757503e-05), math.log(0.0002))), 1.9999999494757503e-05, 0.0002),
        "wattage_per_category": jnp.clip(jnp.exp(jax.random.uniform(seeds[6], (POWER_LEVELS,), jnp.float32, math.log(1.9999999949504854e-06), math.log(1.9999999494757503e-05))), 1.9999999949504854e-06, 1.9999999494757503e-05),
    }


def previous(values, dimension):
    widths = [(0, 0)] * values.ndim
    widths[dimension] = (1, 0)
    return lax.slice_in_dim(jnp.pad(values, widths), 0, values.shape[dimension], axis=dimension)


def following(values, dimension):
    widths = [(0, 0)] * values.ndim
    widths[dimension] = (0, 1)
    return lax.slice_in_dim(jnp.pad(values, widths), 1, values.shape[dimension] + 1, axis=dimension)


def stencil(lateral, vertical, capacity_diagonal, inside, factor):
    row_before = factor * 0.5 * (lateral + previous(lateral, 1))
    row_after = factor * 0.5 * (lateral + following(lateral, 1))
    col_before = factor * 0.5 * (lateral + previous(lateral, 2))
    col_after = factor * 0.5 * (lateral + following(lateral, 2))
    faces = 0.5 * (vertical[1:] + vertical[:-1])
    no_face = jnp.zeros_like(vertical[:1])
    layer_below = jnp.concatenate([no_face, faces], 0)
    layer_above = jnp.concatenate([faces, no_face], 0)
    diagonal = capacity_diagonal + row_before + row_after + col_before + col_after + layer_below + layer_above
    diagonal = jnp.where(inside > 0, diagonal, 1.0)
    return (row_before, row_after, col_before, col_after, layer_below, layer_above, diagonal)


def coupled(values, weights):
    summed = weights[0] * previous(values, 1) + weights[1] * following(values, 1)
    summed = summed + weights[2] * previous(values, 2) + weights[3] * following(values, 2)
    return summed + weights[4] * previous(values, 0) + weights[5] * following(values, 0)


def parity(extent):
    summed = lax.broadcasted_iota(jnp.int32, extent, 0) + lax.broadcasted_iota(jnp.int32, extent, 1)
    return (summed + lax.broadcasted_iota(jnp.int32, extent, 2)) % 2


def restrict(values):
    layers, height, breadth = values.shape
    blocks = values.reshape(layers, height // 2, 2, breadth // 2, 2)
    return (blocks[:, :, 0, :, 0] + blocks[:, :, 1, :, 0] + blocks[:, :, 0, :, 1] + blocks[:, :, 1, :, 1]) * 0.25


def prolong(values):
    return jnp.repeat(jnp.repeat(values, 2, axis=1), 2, axis=2)


def lookup(labels, entries):
    summed = jnp.zeros(labels.shape, entries.dtype)
    for number in range(entries.shape[0]):
        summed = summed + jnp.where(labels == number, entries[number], 0.0)
    return summed


def conjugate(source_vector, weights):
    solution = jnp.zeros_like(source_vector)
    residue = source_vector
    precond = residue / weights[6]
    search = precond
    inner = jnp.sum(residue * precond)
    for step_index in range(COARSE_ITERS):
        image = weights[6] * search - coupled(search, weights)
        alpha_step = inner / jnp.sum(search * image)
        solution = solution + alpha_step * search
        residue = residue - alpha_step * image
        precond = residue / weights[6]
        inner_next = jnp.sum(residue * precond)
        search = precond + (inner_next / inner) * search
        inner = inner_next
    return solution


def smooth(present_guess, source_vector, weights, colours):
    for sweep_index in range(SWEEPS):
        for colour in (0, 1):
            candidate = (source_vector + coupled(present_guess, weights)) / weights[6]
            present_guess = jnp.where(colours == colour, candidate, present_guess)
    return present_guess


def reference(earlier_heat_field, substance_per_voxel, patch_wattage_category, planar_coupling, vertical_coupling_per_substance, heat_mass_ratio, wattage_per_category):
    lateral = lookup(substance_per_voxel, planar_coupling)
    vertical = lookup(substance_per_voxel, vertical_coupling_per_substance)
    capacity_diagonal = lookup(substance_per_voxel, heat_mass_ratio)
    heat = jnp.repeat(jnp.repeat(lookup(patch_wattage_category, wattage_per_category), TILE, axis=0), TILE, axis=1)
    source_vector = capacity_diagonal * earlier_heat_field
    source_vector = jnp.concatenate([source_vector[:1] + heat[None], source_vector[1:]], 0)
    coefficients = [(lateral, vertical, capacity_diagonal)]
    for level_index in range(LEVELS):
        last = coefficients[-1]
        coefficients.append((restrict(last[0]), restrict(last[1]), restrict(last[2])))
    present_guess = earlier_heat_field
    saved = []
    for level_index in range(LEVELS):
        level_coef = coefficients[level_index]
        weights = stencil(level_coef[0], level_coef[1], level_coef[2], jnp.ones_like(source_vector), 0.25 ** level_index)
        colours = parity(source_vector.shape)
        present_guess = smooth(present_guess, source_vector, weights, colours)
        residual = source_vector - (weights[6] * present_guess - coupled(present_guess, weights))
        saved.append((present_guess, source_vector, weights, colours))
        source_vector = restrict(residual)
        present_guess = jnp.zeros_like(source_vector)
    coarse_coef = coefficients[LEVELS]
    coarse_weights = stencil(coarse_coef[0], coarse_coef[1], coarse_coef[2], jnp.ones_like(source_vector), 0.25 ** LEVELS)
    correction = conjugate(source_vector, coarse_weights)
    for level_index in reversed(range(LEVELS)):
        present_guess, source_vector, weights, colours = saved[level_index]
        present_guess = smooth(present_guess + prolong(correction), source_vector, weights, colours)
        correction = present_guess
    return correction
```

```python
import functools

import jax
import jax.numpy as jnp
from jax import lax
from jax.experimental import pallas as pl
from jax.experimental.pallas import tpu as pltpu
from jax.sharding import PartitionSpec as P

TILE = 16
LEVELS = 6
SWEEPS = 2
COARSE_ITERS = 12
LOCAL = 3
FRAME = 64
WIDE = 56
PAD = 8
F32 = jnp.float32
VM = 60 * 1024 * 1024


def up_to(count, step):
    return -(-count // step) * step


def spans(low, high, columns):
    step = max(8, 8 * (4096 // columns // 8) * 2)
    return [(r, min(step, high - r)) for r in range(low, high, step)]


def split_dot(matrix_left, values, matrix_right):
    def parts(x):
        a = x.astype(jnp.bfloat16)
        x = x - a.astype(F32)
        b = x.astype(jnp.bfloat16)
        x = x - b.astype(F32)
        return a, b, x.astype(jnp.bfloat16)

    dot = functools.partial(jnp.dot, preferred_element_type=F32)
    a, b, c = parts(values)
    values = (dot(matrix_left, c) + dot(matrix_left, b)) + dot(matrix_left, a)
    a, b, c = parts(values)
    return (dot(c, matrix_right) + dot(b, matrix_right)) + dot(a, matrix_right)


def pairs(rows, columns, weight, tall):
    r = lax.broadcasted_iota(jnp.int32, (rows, columns), 0)
    c = lax.broadcasted_iota(jnp.int32, (rows, columns), 1)
    hit = (r // 2 == c) if tall else (c // 2 == r)
    return jnp.where(hit, F32(weight), F32(0.0)).astype(jnp.bfloat16)


def restrict(fine, coarse, layers_fine, layers_coarse):
    rf, cf = fine.shape[1] - 2 * PAD, fine.shape[2]
    rc, cc = coarse.shape[1] - 2 * PAD, coarse.shape[2]
    left = pairs(rc, rf, 0.5, False)
    right = pairs(cf, cc, 0.5, True)

    def body(k, carry):
        x = fine[k + layers_fine, PAD : PAD + rf, :]
        coarse[k + layers_coarse, PAD : PAD + rc, :] = split_dot(left, x, right)
        return carry

    lax.fori_loop(0, 6, body, 0)


def prolong_add(coarse, fine):
    rf, cf = fine.shape[1] - 2 * PAD, fine.shape[2]
    rc, cc = coarse.shape[1] - 2 * PAD, coarse.shape[2]
    left = pairs(rf, rc, 1.0, True)
    right = pairs(cc, cf, 1.0, False)

    def body(k, carry):
        x = coarse[k + 1, PAD : PAD + rc, :]
        fine[k + 1, PAD : PAD + rf, :] += split_dot(left, x, right)
        return carry

    lax.fori_loop(0, 6, body, 0)


def build(coef, weights, scale):
    lat, ver, sto = coef
    wr, wc, wv, inv, diag = weights
    rows, columns = lat.shape[1] - 2 * PAD, lat.shape[2]
    half = F32(0.5 * scale)
    wr[...] = jnp.zeros_like(wr)
    wv[0] = jnp.zeros(wv.shape[1:], F32)
    wv[6] = jnp.zeros(wv.shape[1:], F32)

    def faces(k, carry):
        for r, n in spans(PAD, PAD + rows, columns):
            here = lat[k, r : r + n, :]
            wr[k, r : r + n, :] = half * (here + lat[k, r - 1 : r - 1 + n, :])
            wc[k, r : r + n, :] = half * (here + pltpu.roll(here, 1, 1))
        wr[k, PAD + rows : PAD + rows + 8, :] = half * (
            lat[k, PAD + rows : PAD + rows + 8, :]
            + lat[k, PAD + rows - 1 : PAD + rows + 7, :]
        )
        return carry

    lax.fori_loop(0, 6, faces, 0)

    def layer(k, carry):
        for r, n in spans(PAD, PAD + rows, columns):
            wv[k, r : r + n, :] = F32(0.5) * (ver[k, r : r + n, :] + ver[k - 1, r : r + n, :])
        return carry

    lax.fori_loop(1, 6, layer, 0)

    def total(k, carry):
        for r, n in spans(PAD, PAD + rows, columns):
            left = wc[k, r : r + n, :]
            s = sto[k, r : r + n, :]
            d = s + wr[k, r : r + n, :] + wr[k, r + 1 : r + 1 + n, :]
            d = d + left + pltpu.roll(left, columns - 1, 1)
            d = d + wv[k, r : r + n, :] + wv[k + 1, r : r + n, :]
            diag[k, r : r + n, :] = d
            inv[k, r : r + n, :] = jnp.where(s > 0.0, F32(1.0) / jnp.where(s > 0.0, d, 1.0), 0.0)
        return carry

    lax.fori_loop(0, 6, total, 0)


def beside(u, weights, k, r, n, here):
    wr, wc, wv = weights[:3]
    columns = u.shape[2]
    left = wc[k, r : r + n, :]
    summed = wr[k, r : r + n, :] * u[k + 1, r - 1 : r - 1 + n, :]
    summed += wr[k, r + 1 : r + 1 + n, :] * u[k + 1, r + 1 : r + 1 + n, :]
    summed += left * pltpu.roll(here, 1, 1)
    summed += pltpu.roll(left * here, columns - 1, 1)
    summed += wv[k, r : r + n, :] * u[k, r : r + n, :]
    summed += wv[k + 1, r : r + n, :] * u[k + 2, r : r + n, :]
    return summed


def smooth(u, rhs, weights, low, high):
    inv = weights[3]
    columns = u.shape[2]

    def half_sweep(step, carry):
        colour = step % 2

        def layer(k, inner):
            for r, n in spans(PAD + low, PAD + high, columns):
                here = u[k + 1, r : r + n, :]
                new = (rhs[k, r : r + n, :] + beside(u, weights, k, r, n, here)) * inv[
                    k, r : r + n, :
                ]
                odd = lax.broadcasted_iota(jnp.int32, (n, columns), 0)
                odd = (odd + lax.broadcasted_iota(jnp.int32, (n, columns), 1) + k + colour) & 1
                u[k + 1, r : r + n, :] = jnp.where(odd == 0, new, here)
            return inner

        return lax.fori_loop(0, 6, layer, carry)

    lax.fori_loop(0, 2 * SWEEPS, half_sweep, 0)


def residual(u, rhs, weights, out):
    diag = weights[4]
    rows, columns = u.shape[1] - 2 * PAD, u.shape[2]

    def layer(k, carry):
        for r, n in spans(PAD, PAD + rows, columns):
            here = u[k + 1, r : r + n, :]
            out[k, r : r + n, :] = rhs[k, r : r + n, :] - (
                diag[k, r : r + n, :] * here - beside(u, weights, k, r, n, here)
            )
        return carry

    lax.fori_loop(0, 6, layer, 0)


def down_level(index, u, rhs, coef, weights, temp, nxt_rhs, nxt_coef, low, high):
    if index > 0:
        u[...] = jnp.zeros_like(u)
    build(coef, weights, 0.25**index)
    smooth(u, rhs, weights, low, high)
    residual(u, rhs, weights, temp)
    restrict(temp, nxt_rhs, 0, 0)
    for mine, following in zip(coef, nxt_coef):
        following[...] = jnp.zeros_like(following)
        restrict(mine, following, 0, 0)


def down_kernel(x_ref, lat_t, ver_t, sto_t, *refs):
    outs, scratch = refs[: 6 * LOCAL + 4], refs[6 * LOCAL + 4 :]
    level = [outs[6 * i : 6 * i + 6] for i in range(LOCAL)]
    coarse = outs[6 * LOCAL :]
    own = [scratch[5 * i : 5 * i + 5] for i in range(LOCAL)]
    u, rhs = level[0][:2]
    lat, ver, sto = own[0][:3]
    rows, columns = x_ref.shape[1:]
    for ref in (u, lat):
        ref[...] = jnp.zeros_like(ref)

    def look(k, carry):
        for r, n in spans(0, rows, columns):
            labels = x_ref[k + 6, r : r + n, :]
            a = jnp.zeros((n, columns), F32)
            b, c = a, a
            for m in range(lat_t.shape[0]):
                hit = labels == F32(m + 1)
                a = jnp.where(hit, lat_t[m], a)
                b = jnp.where(hit, ver_t[m], b)
                c = jnp.where(hit, sto_t[m], c)
            t = x_ref[k, r : r + n, :]
            lat[k, r + PAD : r + PAD + n, :] = a
            ver[k, r + PAD : r + PAD + n, :] = b
            sto[k, r + PAD : r + PAD + n, :] = c
            u[k + 1, r + PAD : r + PAD + n, :] = t
            rhs[k, r + PAD : r + PAD + n, :] = c * t
        return carry

    lax.fori_loop(0, 6, look, 0)
    rhs[0, PAD : PAD + rows, :] += x_ref[12]
    for i in range(LOCAL):
        last = i == LOCAL - 1
        size = level[i][0].shape[1] - 2 * PAD
        cut = 8 if i < 2 else 0
        down_level(
            i,
            level[i][0],
            level[i][1],
            own[i][:3],
            level[i][2:6] + own[i][3:4],
            own[i][4],
            coarse[0] if last else level[i + 1][1],
            coarse[1:4] if last else own[i + 1][:3],
            cut,
            size - cut,
        )


def coarse_kernel(g_ref, out_ref, *scratch):
    count = LEVELS - LOCAL
    rows, columns = g_ref.shape[1:]
    data = [scratch[11 * i : 11 * i + 11] for i in range(count + 1)]
    for j in range(4):
        ref = data[0][(1, 6, 7, 8)[j]]
        ref[...] = jnp.zeros_like(ref)

        def take(k, carry, ref=ref, j=j):
            ref[k, PAD : PAD + rows, :] = g_ref[6 * j + k]
            return carry

        lax.fori_loop(0, 6, take, 0)
    for i in range(count):
        u, rhs, wr, wc, wv, inv, lat, ver, sto, diag, temp = data[i]
        down_level(
            LOCAL + i, u, rhs, (lat, ver, sto), (wr, wc, wv, inv, diag), temp,
            data[i + 1][1], data[i + 1][6:9], 0, u.shape[1] - 2 * PAD,
        )
    u, rhs, wr, wc, wv, inv, lat, ver, sto, diag, temp = data[count]
    build((lat, ver, sto), (wr, wc, wv, inv, diag), 0.25**LEVELS)
    n, columns = u.shape[1] - 2 * PAD, u.shape[2]
    u[...] = jnp.zeros_like(u)
    mid = slice(PAD, PAD + n)

    def summed(x):
        x = jnp.sum(x, axis=0)
        return jnp.sum(jnp.sum(x, axis=0, keepdims=True), axis=1, keepdims=True)

    r0 = rhs[:, mid, :]
    z0 = r0 * inv[:, mid, :]
    u[1:7, mid, :] = z0
    temp[:, mid, :] = r0
    lat[:, mid, :] = jnp.zeros_like(r0)

    def step(_, rz):
        p = u[1:7, mid, :]
        image = jnp.stack(
            [diag[k, mid, :] * p[k] - beside(u, (wr, wc, wv), k, PAD, n, p[k]) for k in range(6)]
        )
        alpha = rz / summed(p * image)
        lat[:, mid, :] += alpha[None] * p
        r = temp[:, mid, :] - alpha[None] * image
        temp[:, mid, :] = r
        z = r * inv[:, mid, :]
        rz_new = summed(r * z)
        u[1:7, mid, :] = z + (rz_new / rz)[None] * p
        return rz_new

    lax.fori_loop(0, COARSE_ITERS, step, summed(r0 * z0))
    u[1:7, mid, :] = lat[:, mid, :]
    for i in reversed(range(count)):
        u, rhs, wr, wc, wv, inv = data[i][:6]
        prolong_add(data[i + 1][0], u)
        smooth(u, rhs, (wr, wc, wv, inv), 0, u.shape[1] - 2 * PAD)
    u = data[0][0]

    def give(k, carry):
        out_ref[k] = u[k + 1, PAD : PAD + rows, :]
        return carry

    lax.fori_loop(0, 6, give, 0)


def up_kernel(e_ref, *refs):
    ins = refs[: 6 * LOCAL]
    out_ref = refs[6 * LOCAL]
    us = refs[6 * LOCAL + 1 :]
    correction = e_ref
    for i in reversed(range(LOCAL)):
        u, rhs, wr, wc, wv, inv = ins[6 * i : 6 * i + 6]
        mine = us[i]
        mine[...] = u[...]
        prolong_add(correction, mine)
        size = u.shape[1] - 2 * PAD
        cut = (56, 24, 8)[i]
        smooth(mine, rhs, (wr, wc, wv, inv), cut, size - cut)
        correction = mine
    rows, columns = out_ref.shape[1:]
    wide = correction.shape[2]

    def give(k, carry):
        x = correction[k + 1, PAD + FRAME : PAD + FRAME + rows, :]
        out_ref[k] = pltpu.roll(x, wide - FRAME, 1)[:, :columns]
        return carry

    lax.fori_loop(0, 6, give, 0)


def extended(block, axis, dim):
    count = lax.axis_size(axis)
    forward = [(i, i + 1) for i in range(count - 1)]
    backward = [(target, source) for source, target in forward]
    size = block.shape[dim]
    low = lax.ppermute(lax.slice_in_dim(block, size - WIDE, None, axis=dim), axis, forward)
    high = lax.ppermute(lax.slice_in_dim(block, 0, WIDE, axis=dim), axis, backward)
    shape = list(block.shape)
    shape[dim] = FRAME - WIDE
    edge = jnp.zeros(shape, block.dtype)
    return jnp.concatenate([edge, low, block, high, edge], axis=dim)


def lookup(labels, entries):
    summed = jnp.zeros(labels.shape, entries.dtype)
    for number in range(entries.shape[0]):
        summed = summed + jnp.where(labels == number, entries[number], 0.0)
    return summed


def frame(layers, rows, columns):
    return (layers, rows + 2 * PAD, columns)


def on_device(field, substance, patch, planar, vertical, storage, wattage):
    heat = jnp.repeat(jnp.repeat(lookup(patch, wattage), TILE, axis=0), TILE, axis=1)
    x = jnp.concatenate([field, substance.astype(F32) + 1.0, heat[None]], 0)
    x = extended(extended(x, "gy", 2), "gx", 1)
    local_rows, local_cols = field.shape[1:]
    vmem = pl.BlockSpec(memory_space=pltpu.VMEM)
    smem = pl.BlockSpec(memory_space=pltpu.SMEM)
    params = pltpu.CompilerParams(vmem_limit_bytes=VM)
    dims = []
    for i in range(LOCAL + 1):
        dims.append(
            (
                up_to((local_rows + 2 * FRAME) >> i, 8),
                up_to((local_cols + 2 * FRAME) >> i, 128),
            )
        )
    shapes, scratch = [], []
    for i in range(LOCAL):
        shapes += [jax.ShapeDtypeStruct(frame(n, *dims[i]), F32) for n in (8, 6, 6, 6, 7, 6)]
        scratch += [pltpu.VMEM(frame(6, *dims[i]), F32) for _ in range(5)]
    coarse = [jax.ShapeDtypeStruct(frame(6, *dims[LOCAL]), F32)] * 4
    result = pl.pallas_call(
        down_kernel,
        out_shape=shapes + coarse,
        in_specs=[vmem] + [smem] * 3,
        out_specs=[vmem] * (6 * LOCAL + 4),
        scratch_shapes=scratch,
        compiler_params=params,
    )(x, planar, vertical, storage)
    levels, coarse = result[: 6 * LOCAL], result[6 * LOCAL :]
    h, w = local_rows >> LOCAL, local_cols >> LOCAL
    off = FRAME >> LOCAL
    mine = jnp.concatenate(
        [c[:, PAD + off : PAD + off + h, off : off + w] for c in coarse], 0
    )
    nx, ny = lax.axis_size("gx"), lax.axis_size("gy")
    all_blocks = lax.all_gather(mine, ("gx", "gy"), axis=0, tiled=False)
    all_blocks = all_blocks.reshape(nx, ny, 24, h, w).transpose(2, 0, 3, 1, 4)
    whole = all_blocks.reshape(24, nx * h, ny * w)
    sizes = [
        (up_to(((nx * h) >> i) + 1, 8), up_to(((ny * w) >> i) + 1, 128))
        for i in range(LEVELS - LOCAL + 1)
    ]
    whole = jnp.pad(
        whole, ((0, 0), (0, sizes[0][0] - nx * h), (0, sizes[0][1] - ny * w))
    )
    scratch = []
    for size in sizes:
        scratch += [
            pltpu.VMEM(frame(n, *size), F32) for n in (8, 6, 6, 6, 7, 6, 6, 6, 6, 6, 6)
        ]
    solved = pl.pallas_call(
        coarse_kernel,
        out_shape=jax.ShapeDtypeStruct((6,) + sizes[0], F32),
        in_specs=[vmem],
        out_specs=vmem,
        scratch_shapes=scratch,
        compiler_params=params,
    )(whole)
    solved = jnp.pad(solved, ((1, 1), (off, off), (off, off)))
    zero = jnp.int32(0)
    window = lax.dynamic_slice(
        solved,
        (zero, lax.axis_index("gx") * h, lax.axis_index("gy") * w),
        (8, h + 2 * off, w + 2 * off),
    )
    r3, c3 = dims[LOCAL]
    window = jnp.pad(window, ((0, 0), (PAD, PAD), (0, c3 - (w + 2 * off))))
    return pl.pallas_call(
        up_kernel,
        out_shape=jax.ShapeDtypeStruct(field.shape, F32),
        in_specs=[vmem] * (1 + 6 * LOCAL),
        out_specs=vmem,
        scratch_shapes=[pltpu.VMEM(frame(8, *dims[i]), F32) for i in range(LOCAL)],
        compiler_params=params,
    )(window, *levels)


def solution(mesh):
    placed = (P(None, "gx", "gy"), P(None, "gx", "gy"), P("gx", "gy"), P(), P(), P(), P())
    return jax.shard_map(
        on_device, mesh=mesh, in_specs=placed, out_specs=P(None, "gx", "gy"), check_vma=False
    )
```

```python
import functools

import jax
import jax.numpy as jnp
from jax import lax
from jax.experimental import pallas as pl
from jax.experimental.pallas import tpu as pltpu
from jax.sharding import PartitionSpec as P

TILE = 16
LEVELS = 6
SWEEPS = 2
COARSE_ITERS = 12
LOCAL = 3
FRAME = 64
WIDE = 56
PAD = 8
F32 = jnp.float32
VM = 60 * 1024 * 1024


def up_to(count, step):
    return -(-count // step) * step


def spans(low, high, columns):
    step = max(8, 8 * (4096 // columns // 8) * 2)
    return [(r, min(step, high - r)) for r in range(low, high, step)]


def split_dot(matrix_left, values, matrix_right):
    def parts(x):
        a = x.astype(jnp.bfloat16)
        x = x - a.astype(F32)
        b = x.astype(jnp.bfloat16)
        x = x - b.astype(F32)
        return a, b, x.astype(jnp.bfloat16)

    dot = functools.partial(jnp.dot, preferred_element_type=F32)
    a, b, c = parts(values)
    values = (dot(matrix_left, c) + dot(matrix_left, b)) + dot(matrix_left, a)
    a, b, c = parts(values)
    return (dot(c, matrix_right) + dot(b, matrix_right)) + dot(a, matrix_right)


def pairs(rows, columns, weight, tall):
    r = lax.broadcasted_iota(jnp.int32, (rows, columns), 0)
    c = lax.broadcasted_iota(jnp.int32, (rows, columns), 1)
    hit = (r // 2 == c) if tall else (c // 2 == r)
    return jnp.where(hit, F32(weight), F32(0.0)).astype(jnp.bfloat16)


def restrict(fine, coarse, layers_fine, layers_coarse):
    rf, cf = fine.shape[1] - 2 * PAD, fine.shape[2]
    rc, cc = coarse.shape[1] - 2 * PAD, coarse.shape[2]
    left = pairs(rc, rf, 0.5, False)
    right = pairs(cf, cc, 0.5, True)

    def body(k, carry):
        x = fine[k + layers_fine, PAD : PAD + rf, :]
        coarse[k + layers_coarse, PAD : PAD + rc, :] = split_dot(left, x, right)
        return carry

    lax.fori_loop(0, 6, body, 0)


def prolong_add(coarse, fine):
    rf, cf = fine.shape[1] - 2 * PAD, fine.shape[2]
    rc, cc = coarse.shape[1] - 2 * PAD, coarse.shape[2]
    left = pairs(rf, rc, 1.0, True)
    right = pairs(cc, cf, 1.0, False)

    def body(k, carry):
        x = coarse[k + 1, PAD : PAD + rc, :]
        fine[k + 1, PAD : PAD + rf, :] += split_dot(left, x, right)
        return carry

    lax.fori_loop(0, 6, body, 0)


def build(coef, weights, scale):
    lat, ver, sto = coef
    wr, wc, wv, inv, diag = weights
    rows, columns = lat.shape[1] - 2 * PAD, lat.shape[2]
    half = F32(0.5 * scale)
    wr[...] = jnp.zeros_like(wr)
    wv[0] = jnp.zeros(wv.shape[1:], F32)
    wv[6] = jnp.zeros(wv.shape[1:], F32)

    def faces(k, carry):
        for r, n in spans(PAD, PAD + rows, columns):
            here = lat[k, r : r + n, :]
            wr[k, r : r + n, :] = half * (here + lat[k, r - 1 : r - 1 + n, :])
            wc[k, r : r + n, :] = half * (here + pltpu.roll(here, 1, 1))
        wr[k, PAD + rows : PAD + rows + 8, :] = half * (
            lat[k, PAD + rows : PAD + rows + 8, :]
            + lat[k, PAD + rows - 1 : PAD + rows + 7, :]
        )
        return carry

    lax.fori_loop(0, 6, faces, 0)

    def layer(k, carry):
        for r, n in spans(PAD, PAD + rows, columns):
            wv[k, r : r + n, :] = F32(0.5) * (ver[k, r : r + n, :] + ver[k - 1, r : r + n, :])
        return carry

    lax.fori_loop(1, 6, layer, 0)

    def total(k, carry):
        for r, n in spans(PAD, PAD + rows, columns):
            left = wc[k, r : r + n, :]
            s = sto[k, r : r + n, :]
            d = s + wr[k, r : r + n, :] + wr[k, r + 1 : r + 1 + n, :]
            d = d + left + pltpu.roll(left, columns - 1, 1)
            d = d + wv[k, r : r + n, :] + wv[k + 1, r : r + n, :]
            diag[k, r : r + n, :] = d
            inv[k, r : r + n, :] = jnp.where(s > 0.0, F32(1.0) / jnp.where(s > 0.0, d, 1.0), 0.0)
        return carry

    lax.fori_loop(0, 6, total, 0)


def beside(u, weights, k, r, n, here):
    wr, wc, wv = weights[:3]
    columns = u.shape[2]
    left = wc[k, r : r + n, :]
    summed = wr[k, r : r + n, :] * u[k + 1, r - 1 : r - 1 + n, :]
    summed += wr[k, r + 1 : r + 1 + n, :] * u[k + 1, r + 1 : r + 1 + n, :]
    summed += left * pltpu.roll(here, 1, 1)
    summed += pltpu.roll(left * here, columns - 1, 1)
    summed += wv[k, r : r + n, :] * u[k, r : r + n, :]
    summed += wv[k + 1, r : r + n, :] * u[k + 2, r : r + n, :]
    return summed


def smooth(u, rhs, weights, low, high):
    inv = weights[3]
    columns = u.shape[2]

    def half_sweep(step, carry):
        colour = step % 2

        def layer(k, inner):
            for r, n in spans(PAD + low, PAD + high, columns):
                here = u[k + 1, r : r + n, :]
                new = (rhs[k, r : r + n, :] + beside(u, weights, k, r, n, here)) * inv[
                    k, r : r + n, :
                ]
                odd = lax.broadcasted_iota(jnp.int32, (n, columns), 0)
                odd = (odd + lax.broadcasted_iota(jnp.int32, (n, columns), 1) + k + colour) & 1
                u[k + 1, r : r + n, :] = jnp.where(odd == 0, new, here)
            return inner

        return lax.fori_loop(0, 6, layer, carry)

    lax.fori_loop(0, 2 * SWEEPS, half_sweep, 0)


def residual(u, rhs, weights, out):
    diag = weights[4]
    rows, columns = u.shape[1] - 2 * PAD, u.shape[2]

    def layer(k, carry):
        for r, n in spans(PAD, PAD + rows, columns):
            here = u[k + 1, r : r + n, :]
            out[k, r : r + n, :] = rhs[k, r : r + n, :] - (
                diag[k, r : r + n, :] * here - beside(u, weights, k, r, n, here)
            )
        return carry

    lax.fori_loop(0, 6, layer, 0)


def down_level(index, u, rhs, coef, weights, temp, nxt_rhs, nxt_coef, low, high):
    if index > 0:
        u[...] = jnp.zeros_like(u)
    build(coef, weights, 0.25**index)
    smooth(u, rhs, weights, low, high)
    residual(u, rhs, weights, temp)
    restrict(temp, nxt_rhs, 0, 0)
    for mine, following in zip(coef, nxt_coef):
        following[...] = jnp.zeros_like(following)
        restrict(mine, following, 0, 0)


def down_kernel(x_ref, lat_t, ver_t, sto_t, *refs):
    outs, packed, scratch = refs[: 6 * LOCAL], refs[6 * LOCAL], refs[6 * LOCAL + 1 :]
    level = [outs[6 * i : 6 * i + 6] for i in range(LOCAL)]
    coarse = scratch[5 * LOCAL :]
    own = [scratch[5 * i : 5 * i + 5] for i in range(LOCAL)]
    u, rhs = level[0][:2]
    lat, ver, sto = own[0][:3]
    rows, columns = x_ref.shape[1:]
    for ref in (u, lat):
        ref[...] = jnp.zeros_like(ref)

    def look(k, carry):
        for r, n in spans(0, rows, columns):
            labels = x_ref[k + 6, r : r + n, :]
            a = jnp.zeros((n, columns), F32)
            b, c = a, a
            for m in range(lat_t.shape[0]):
                hit = labels == F32(m + 1)
                a = jnp.where(hit, lat_t[m], a)
                b = jnp.where(hit, ver_t[m], b)
                c = jnp.where(hit, sto_t[m], c)
            t = x_ref[k, r : r + n, :]
            lat[k, r + PAD : r + PAD + n, :] = a
            ver[k, r + PAD : r + PAD + n, :] = b
            sto[k, r + PAD : r + PAD + n, :] = c
            u[k + 1, r + PAD : r + PAD + n, :] = t
            rhs[k, r + PAD : r + PAD + n, :] = c * t
        return carry

    lax.fori_loop(0, 6, look, 0)
    rhs[0, PAD : PAD + rows, :] += x_ref[12]
    for i in range(LOCAL):
        last = i == LOCAL - 1
        size = level[i][0].shape[1] - 2 * PAD
        cut = 8 if i < 2 else 0
        down_level(
            i,
            level[i][0],
            level[i][1],
            own[i][:3],
            level[i][2:6] + own[i][3:4],
            own[i][4],
            coarse[0] if last else level[i + 1][1],
            coarse[1:4] if last else own[i + 1][:3],
            cut,
            size - cut,
        )
    per, h, lanes = packed.shape
    off = FRAME >> LOCAL
    w = lanes * per // 24
    lane = lax.broadcasted_iota(jnp.int32, (h, lanes), 1) // w
    for i in range(per):
        total = jnp.zeros((h, lanes), F32)
        for j in range(24 // per):
            at = j * per + i
            x = coarse[at // 6][at % 6, PAD + off : PAD + off + h, :]
            total = jnp.where(lane == j, pltpu.roll(x, (j * w - off) % lanes, 1), total)
        packed[i] = total


def coarse_kernel(rows_of, g_ref, out_ref, *scratch):
    count = LEVELS - LOCAL
    blocks, per, h, lanes = g_ref.shape
    w = lanes * per // 24
    columns_of = blocks // rows_of
    rows = rows_of * h
    data = [scratch[11 * i : 11 * i + 11] for i in range(count + 1)]
    for j in range(4):
        ref = data[0][(1, 6, 7, 8)[j]]
        ref[...] = jnp.zeros_like(ref)
    lane = lax.broadcasted_iota(jnp.int32, (h, lanes), 1) // w

    def take(gx, carry):
        row = pl.multiple_of(PAD + gx * h, 8)
        for at in range(24):
            j, i = at // per, at % per
            ref = data[0][(1, 6, 7, 8)[at // 6]]
            for start in range(0, columns_of, lanes // w):
                total = jnp.zeros((h, lanes), F32)
                for gy in range(start, min(start + lanes // w, columns_of)):
                    x = g_ref[gx * columns_of + gy, i]
                    x = pltpu.roll(x, ((gy - start - j) * w) % lanes, 1)
                    total = jnp.where(lane == gy - start, x, total)
                ref[at % 6, pl.ds(row, h), start * w : start * w + lanes] = total
        return carry

    lax.fori_loop(0, rows_of, take, 0)
    for i in range(count):
        u, rhs, wr, wc, wv, inv, lat, ver, sto, diag, temp = data[i]
        down_level(
            LOCAL + i, u, rhs, (lat, ver, sto), (wr, wc, wv, inv, diag), temp,
            data[i + 1][1], data[i + 1][6:9], 0, u.shape[1] - 2 * PAD,
        )
    u, rhs, wr, wc, wv, inv, lat, ver, sto, diag, temp = data[count]
    build((lat, ver, sto), (wr, wc, wv, inv, diag), 0.25**LEVELS)
    n, columns = u.shape[1] - 2 * PAD, u.shape[2]
    u[...] = jnp.zeros_like(u)
    mid = slice(PAD, PAD + n)

    def summed(x):
        x = jnp.sum(x, axis=0)
        return jnp.sum(jnp.sum(x, axis=0, keepdims=True), axis=1, keepdims=True)

    r0 = rhs[:, mid, :]
    z0 = r0 * inv[:, mid, :]
    u[1:7, mid, :] = z0
    temp[:, mid, :] = r0
    lat[:, mid, :] = jnp.zeros_like(r0)

    def step(_, rz):
        p = u[1:7, mid, :]
        image = jnp.stack(
            [diag[k, mid, :] * p[k] - beside(u, (wr, wc, wv), k, PAD, n, p[k]) for k in range(6)]
        )
        alpha = rz / summed(p * image)
        lat[:, mid, :] += alpha[None] * p
        r = temp[:, mid, :] - alpha[None] * image
        temp[:, mid, :] = r
        z = r * inv[:, mid, :]
        rz_new = summed(r * z)
        u[1:7, mid, :] = z + (rz_new / rz)[None] * p
        return rz_new

    lax.fori_loop(0, COARSE_ITERS, step, summed(r0 * z0))
    u[1:7, mid, :] = lat[:, mid, :]
    for i in reversed(range(count)):
        u, rhs, wr, wc, wv, inv = data[i][:6]
        prolong_add(data[i + 1][0], u)
        smooth(u, rhs, (wr, wc, wv, inv), 0, u.shape[1] - 2 * PAD)
    u = data[0][0]

    def give(k, carry):
        out_ref[k] = u[k + 1, PAD : PAD + out_ref.shape[1], :]
        return carry

    lax.fori_loop(0, 6, give, 0)


def up_kernel(e_ref, *refs):
    ins = refs[: 6 * LOCAL]
    out_ref = refs[6 * LOCAL]
    us = refs[6 * LOCAL + 1 :]
    correction = e_ref
    for i in reversed(range(LOCAL)):
        u, rhs, wr, wc, wv, inv = ins[6 * i : 6 * i + 6]
        mine = us[i]
        mine[...] = u[...]
        prolong_add(correction, mine)
        size = u.shape[1] - 2 * PAD
        cut = (56, 24, 8)[i]
        smooth(mine, rhs, (wr, wc, wv, inv), cut, size - cut)
        correction = mine
    rows, columns = out_ref.shape[1:]
    wide = correction.shape[2]

    def give(k, carry):
        x = correction[k + 1, PAD + FRAME : PAD + FRAME + rows, :]
        out_ref[k] = pltpu.roll(x, wide - FRAME, 1)[:, :columns]
        return carry

    lax.fori_loop(0, 6, give, 0)


def extended(block, axis, dim):
    count = lax.axis_size(axis)
    forward = [(i, i + 1) for i in range(count - 1)]
    backward = [(target, source) for source, target in forward]
    size = block.shape[dim]
    low = lax.ppermute(lax.slice_in_dim(block, size - WIDE, None, axis=dim), axis, forward)
    high = lax.ppermute(lax.slice_in_dim(block, 0, WIDE, axis=dim), axis, backward)
    shape = list(block.shape)
    shape[dim] = FRAME - WIDE
    edge = jnp.zeros(shape, block.dtype)
    return jnp.concatenate([edge, low, block, high, edge], axis=dim)


def lookup(labels, entries):
    summed = jnp.zeros(labels.shape, entries.dtype)
    for number in range(entries.shape[0]):
        summed = summed + jnp.where(labels == number, entries[number], 0.0)
    return summed


def frame(layers, rows, columns):
    return (layers, rows + 2 * PAD, columns)


def on_device(field, substance, patch, planar, vertical, storage, wattage):
    small = lax.optimization_barrier(lookup(patch, wattage))
    tall = jnp.repeat(jnp.eye(patch.shape[0], dtype=F32), TILE, axis=0)
    flat = jnp.repeat(jnp.eye(patch.shape[1], dtype=F32), TILE, axis=1)
    exact = functools.partial(jnp.dot, precision=lax.Precision.HIGHEST)
    heat = exact(exact(tall, small), flat)
    x = jnp.concatenate([field, substance.astype(F32) + 1.0, heat[None]], 0)
    x = extended(extended(x, "gy", 2), "gx", 1)
    local_rows, local_cols = field.shape[1:]
    vmem = pl.BlockSpec(memory_space=pltpu.VMEM)
    smem = pl.BlockSpec(memory_space=pltpu.SMEM)
    params = pltpu.CompilerParams(vmem_limit_bytes=VM)
    dims = []
    for i in range(LOCAL + 1):
        dims.append(
            (
                up_to((local_rows + 2 * FRAME) >> i, 8),
                up_to((local_cols + 2 * FRAME) >> i, 128),
            )
        )
    shapes, scratch = [], []
    for i in range(LOCAL):
        shapes += [jax.ShapeDtypeStruct(frame(n, *dims[i]), F32) for n in (8, 6, 6, 6, 7, 6)]
        scratch += [pltpu.VMEM(frame(6, *dims[i]), F32) for _ in range(5)]
    scratch += [pltpu.VMEM(frame(6, *dims[LOCAL]), F32) for _ in range(4)]
    h, w = local_rows >> LOCAL, local_cols >> LOCAL
    off = FRAME >> LOCAL
    lanes = dims[LOCAL][1]
    result = pl.pallas_call(
        down_kernel,
        out_shape=shapes + [jax.ShapeDtypeStruct((24 * w // lanes, h, lanes), F32)],
        in_specs=[vmem] + [smem] * 3,
        out_specs=[vmem] * (6 * LOCAL + 1),
        scratch_shapes=scratch,
        compiler_params=params,
    )(x, planar, vertical, storage)
    levels, mine = result[: 6 * LOCAL], result[6 * LOCAL]
    nx, ny = lax.axis_size("gx"), lax.axis_size("gy")
    whole = lax.all_gather(mine, ("gx", "gy"), axis=0, tiled=False)
    sizes = [
        (up_to(((nx * h) >> i) + 1, 8), up_to(((ny * w) >> i) + 1, 128))
        for i in range(LEVELS - LOCAL + 1)
    ]
    scratch = []
    for size in sizes:
        scratch += [
            pltpu.VMEM(frame(n, *size), F32) for n in (8, 6, 6, 6, 7, 6, 6, 6, 6, 6, 6)
        ]
    solved = pl.pallas_call(
        functools.partial(coarse_kernel, nx),
        out_shape=jax.ShapeDtypeStruct((6,) + sizes[0], F32),
        in_specs=[vmem],
        out_specs=vmem,
        scratch_shapes=scratch,
        compiler_params=params,
    )(whole)
    solved = jnp.pad(solved, ((1, 1), (off, off), (off, off)))
    zero = jnp.int32(0)
    window = lax.dynamic_slice(
        solved,
        (zero, lax.axis_index("gx") * h, lax.axis_index("gy") * w),
        (8, h + 2 * off, w + 2 * off),
    )
    r3, c3 = dims[LOCAL]
    window = jnp.pad(window, ((0, 0), (PAD, PAD), (0, c3 - (w + 2 * off))))
    return pl.pallas_call(
        up_kernel,
        out_shape=jax.ShapeDtypeStruct(field.shape, F32),
        in_specs=[vmem] * (1 + 6 * LOCAL),
        out_specs=vmem,
        scratch_shapes=[pltpu.VMEM(frame(8, *dims[i]), F32) for i in range(LOCAL)],
        compiler_params=params,
    )(window, *levels)


def solution(mesh):
    placed = (P(None, "gx", "gy"), P(None, "gx", "gy"), P("gx", "gy"), P(), P(), P(), P())
    return jax.shard_map(
        on_device, mesh=mesh, in_specs=placed, out_specs=P(None, "gx", "gy"), check_vma=False
    )
```
